256 devices in a mesh: dp: 32 (over z, y_hi, core), mp: 8 (over x, y_lo).
Axes of the slice: x: 4, y: 4 (y_hi: 2, y_lo: 2; y = y_hi * 2 + y_lo), z: 8, core: 2. Of those that a mesh axis runs over, the one named last changes fastest.
Arguments:
- activations: bfloat16 [16384, 28672], P('dp', 'mp'), may hold values from -200 to 200
- weight: bfloat16 [8192, 28672], P(None, ('mp', 'dp')), may hold values from -25 to 25
- thresholds: float32 [8192], P('dp'), may hold values from 0.5 to 1.5
Outputs:
- pruned: bfloat16 [8192, 28672], P('dp', 'mp')
The draws below stay inside these ranges and needn't reach their ends.
All inputs are finite; a program needn't handle non-finite values.
Results may differ from the reference program's by a relative error of at most 0.0004.
Values may be sent and summed in bfloat16 or wider, within the bound.
A program may use at most 64 MiB of HBM per device.

```python
import jax
import jax.numpy as jnp
from jax import lax

OUT = 8192
IN = 28672
TOKENS = 16384
N_DP = 32


def draw_activations(key, part):
    keys = jax.random.split(jax.random.fold_in(key, 11), 3)
    positions = jnp.arange(TOKENS, dtype=jnp.float32)[:, None]
    row_scale = 10.0 ** jax.random.uniform(keys[0], (TOKENS, 1), jnp.float32) * 3.0 ** (positions / TOKENS - 1.0)
    col_scale = 10.0 ** (jax.random.uniform(keys[1], (1, IN), jnp.float32) - 0.5)
    noise = jnp.clip(jax.random.normal(keys[2], (TOKENS, IN), jnp.float32), -4.0, 4.0)
    return (noise * row_scale * col_scale).astype(jnp.bfloat16)


def draw_weight(key, part):
    keys = jax.random.split(jax.random.fold_in(key, 23), 2)
    columns = jnp.arange(IN, dtype=jnp.float32)[None, :]
    col_scale = 10.0 ** (jax.random.uniform(keys[0], (1, IN), jnp.float32) - 0.5) * 3.0 ** (columns / IN - 0.5)
    noise = jnp.clip(jax.random.normal(keys[1], (OUT, IN), jnp.float32), -4.0, 4.0)
    return (noise * col_scale).astype(jnp.bfloat16)


def shard_levels(key, shape, pieces, smallest, top_value):
    level, own = 1.0, jax.random.fold_in(key, 6)
    for position, parts in pieces:
        draws = jnp.exp(jax.random.uniform(jax.random.fold_in(own, position), (parts,), jnp.float32, smallest / len(pieces), top_value / len(pieces)))
        level = level * jnp.repeat(draws, shape[position] // parts).reshape([-1 if axis == position else 1 for axis in range(len(shape))])
    return level


def setup_inputs(seed: int = 0) -> dict:
    seeds = jax.random.split(jax.random.key(seed), 4)
    return {
        "activations": draw_activations(jax.random.fold_in(seeds[3], 71), 0),
        "weight": draw_weight(jax.random.fold_in(seeds[3], 71), 0),
        "thresholds": jnp.clip(0.5 + 1.0 * jax.random.uniform(seeds[2], (OUT,), jnp.float32) ** shard_levels(seeds[2], (OUT,), ((0, 32),), -0.2, 0.2), 0.5, 1.5),
    }


gate_slope = 2.0
small_eps = 1e-06

def reference(activations, weight, thresholds):
    blocks = activations.reshape(N_DP, TOKENS // N_DP, IN)

    def accumulate(total, block):
        return (total + lax.optimization_barrier(jnp.sum(jnp.square(block.astype(jnp.float32)), axis=0)), None)
    squares, _ = lax.scan(accumulate, jnp.zeros((IN,), jnp.float32), blocks)
    col_norm = jnp.sqrt(squares)
    rows = weight.reshape(N_DP, OUT // N_DP, IN)
    limits = thresholds.reshape(N_DP, OUT // N_DP)

    def prune(pair):
        block, limit = pair
        wide = block.astype(jnp.float32)
        scores = jnp.abs(wide) * col_norm[None, :]
        row_mean = lax.optimization_barrier(jnp.sum(scores, axis=1, keepdims=True)) / IN + small_eps
        kept_share = jnp.clip((scores / row_mean - limit[:, None]) * gate_slope + 0.5, 0.0, 1.0)
        return (wide * kept_share).astype(jnp.bfloat16)
    return lax.map(prune, (rows, limits)).reshape(OUT, IN)
```

```python
import functools

import jax
import jax.numpy as jnp
from jax import lax
from jax.experimental import pallas as pl
from jax.experimental.pallas import tpu as pltpu
from jax.sharding import PartitionSpec as P

IN = 28672
LANES = 128
MESH = pl.DeviceIdType.MESH

gate_slope = 2.0
small_eps = 1e-06


FIRST = 9
SECOND = 20


def kernel(
    n_dp, n_mp, act_hbm, wt_hbm, thr_hbm, out_ref,
    act, wt, got, sq_send, sq_got, row_send, row_got, tot_send, tot_got, norms, limits, scale_a, scale_b,
    act_sem, local_sem, bulk_send, bulk_recv, small_send, small_recv,
):
    d, m = lax.axis_index("dp"), lax.axis_index("mp")
    cols, outs = wt_hbm.shape
    rows = outs // n_dp
    groups = n_dp // 8
    per_group = cols * 8 // LANES
    chunks = groups * per_group
    steps = act_sem.shape[0]
    tokens = act_hbm.shape[0] // steps
    depth = n_dp // 4
    peers = n_dp - 1

    z, high, core = lax.div(d, 4), lax.rem(lax.div(d, 2), 2), lax.rem(d, 2)
    sides = ((1 - high) * 2 + core, (1 - high) * 2 + 1 - core, high * 2 + 1 - core, high * 2 + core)
    hops = [depth // 2 + (k // 2 if k % 2 == 0 else -((k + 1) // 2)) for k in range(depth)]
    partners = [(side, hop) for side in range(4) for hop in hops][:-1]

    def target(i):
        side, hop = partners[i]
        return lax.rem(z + hop, depth) * 4 + sides[side]

    def mp_peer(i):
        return lax.rem(m + i, n_mp)

    def act_copy(i):
        span = pl.ds(pl.multiple_of(i * tokens, tokens), tokens)
        return pltpu.make_async_copy(act_hbm.at[span], act.at[span], act_sem.at[i])

    def block(i):
        return pl.ds(pl.multiple_of(i * rows, rows), rows)

    def place_of(i, n=1):
        return pl.ds(pl.multiple_of(i * cols, 16), n * cols)

    def landed(i):
        return bulk_recv.at[min(i // depth, 3) + max(i - 3 * depth, 0)]

    def bulk_copy(i):
        to = target(i)
        return pltpu.make_async_remote_copy(
            src_ref=wt_hbm.at[:, block(to)], dst_ref=got.at[place_of(d)],
            send_sem=bulk_send, recv_sem=landed(i), device_id=(to, m), device_id_type=MESH,
        )

    def small_copy(src, dst, n, i):
        to = target(i)
        return pltpu.make_async_remote_copy(
            src_ref=src.at[to], dst_ref=dst.at[d], send_sem=small_send.at[n], recv_sem=small_recv.at[n],
            device_id=(to, m), device_id_type=MESH,
        )

    def tot_copy(i):
        return pltpu.make_async_remote_copy(
            src_ref=tot_send, dst_ref=tot_got.at[m], send_sem=small_send.at[2], recv_sem=small_recv.at[2],
            device_id=(d, mp_peer(i)), device_id_type=MESH,
        )

    def wait_for(ref, sem):
        pltpu.make_async_copy(ref, ref, sem).wait()

    def loop(lo, hi, body):
        lax.fori_loop(lo, hi, lambda i, c: (body(i), c)[1], 0)

    with jax.named_scope("local"):
        loop(0, steps, lambda i: act_copy(i).start())
        wt_local = pltpu.make_async_copy(wt_hbm, wt, local_sem.at[0])
        wt_local.start()
        own = pltpu.make_async_copy(wt_hbm.at[:, block(d)], got.at[place_of(d)], local_sem.at[1])
        own.start()
        limit_local = pltpu.make_async_copy(thr_hbm, limits, local_sem.at[2])
        limit_local.start()

    with jax.named_scope("signal"):
        barrier = pltpu.get_barrier_semaphore()
        for i in range(peers):
            pl.semaphore_signal(barrier, inc=1, device_id=(target(i), m), device_id_type=MESH)
        for i in range(1, n_mp):
            pl.semaphore_signal(barrier, inc=1, device_id=(d, mp_peer(i)), device_id_type=MESH)

    with jax.named_scope("squares"):
        def add_squares(i, sums):
            act_copy(i).wait()
            base = pl.multiple_of(i * tokens, tokens)
            out = []
            for j in range(chunks):
                x = act[pl.ds(base, tokens), j * LANES:(j + 1) * LANES].astype(jnp.float32)
                out.append(sums[j] + jnp.sum((x * x).reshape(tokens // 8, 8, LANES), axis=0))
            return tuple(out)

        sums = lax.fori_loop(0, steps, add_squares, tuple(jnp.zeros((8, LANES), jnp.float32) for _ in range(chunks)))
        sums = [jnp.sum(s, axis=0, keepdims=True) for s in sums]
        lane = lax.broadcasted_iota(jnp.int32, (1, LANES), 1)
        for q in range(groups):
            for u in range(8):
                shift = (LANES - cols) * u
                first = sums[per_group * q + max(u - 1, 0)]
                second = sums[per_group * q + min(u, per_group - 1)]
                if u:
                    first = pltpu.roll(first, shift, 1)
                    second = pltpu.roll(second, shift, 1)
                row = jnp.where(lane < shift, first, second)
                sq_send[8 * q + u] = jnp.where(lane < cols, row, 0.0)

    with jax.named_scope("barrier"):
        pl.semaphore_wait(barrier, peers + n_mp - 1)

    with jax.named_scope("issue"):
        for i in range(peers):
            small_copy(sq_send, sq_got, 0, i).start()
        for i in range(FIRST):
            bulk_copy(i).start()
        sq_got[d] = sq_send[d]
        wt_local.wait()

    with jax.named_scope("wait_sq"):
        wait_for(sq_got.at[:peers], small_recv.at[0])

    with jax.named_scope("rowpart"):
        squares = jnp.sum(sq_got[...].reshape(n_dp // 8, 8, LANES), axis=0)
        squares = jnp.sum(squares, axis=0, keepdims=True)
        norm = jnp.broadcast_to(jnp.sqrt(squares), (LANES, LANES)).T[:cols]

        def row_part(r):
            for h in range(rows // LANES):
                w = wt[:, pl.ds(pl.multiple_of(r * rows + h * LANES, LANES), LANES)].astype(jnp.float32)
                part = jnp.sum((jnp.abs(w) * norm).reshape(cols // 8, 8, LANES), axis=0)
                row_send[r, :, h * LANES:(h + 1) * LANES] = jnp.sum(part, axis=0, keepdims=True)
            row_send[r, :, rows:] = squares

        loop(0, n_dp, row_part)
    with jax.named_scope("send_row"):
        for i in range(peers):
            small_copy(row_send, row_got, 1, i).start()
        for i in range(FIRST, SECOND):
            bulk_copy(i).start()
        row_got[d] = row_send[d]
    with jax.named_scope("wait_row"):
        wait_for(row_got.at[:peers], small_recv.at[1])

    with jax.named_scope("tot"):
        tot_send[...] = jnp.sum(row_got[:, :, :rows], axis=0)
        for i in range(1, n_mp):
            tot_copy(i).start()
        for i in range(SECOND, peers):
            bulk_copy(i).start()
        tot_got[m] = tot_send[...]
    with jax.named_scope("norms"):
        for q in range(groups):
            for t in range(per_group):
                shift = (LANES - cols) * t
                first = row_got[8 * q + t, :, rows:]
                second = row_got[8 * q + t + 1, :, rows:]
                first = pltpu.roll(first, LANES - shift, 1) if shift else first
                second = pltpu.roll(second, cols - shift, 1)
                norms[per_group * q + t] = jnp.sqrt(jnp.where(lane < cols - shift, first, second))
        limit_local.wait()
        own.wait()
    with jax.named_scope("wait_tot"):
        wait_for(tot_got.at[:n_mp - 1], small_recv.at[2])

    with jax.named_scope("scale"):
        row_mean = jnp.sum(tot_got[...], axis=0) / IN + small_eps
        a = gate_slope / row_mean
        b = 0.5 - gate_slope * limits[...]
        for h in range(rows // LANES):
            part = slice(h * LANES, (h + 1) * LANES)
            scale_a[part] = jnp.broadcast_to(a[:, part], (LANES, LANES)).T
            scale_b[part] = jnp.broadcast_to(b[:, part], (LANES, LANES)).T
        wait_for(sq_got.at[:peers], small_send.at[0])
        wait_for(row_got.at[:peers], small_send.at[1])
        wait_for(tot_got.at[:n_mp - 1], small_send.at[2])

    def finish(j):
        span = pl.ds(pl.multiple_of(j * LANES, LANES), LANES)
        wide = got[span].T.astype(jnp.float32)
        scores = jnp.abs(wide) * norms[j]
        kept = jnp.clip(scores * scale_a[...] + scale_b[...], 0.0, 1.0)
        out_ref[:, span] = (wide * kept).astype(jnp.bfloat16)

    mine = sides[3]
    with jax.named_scope("early"):
        for k in range(3):
            wait_for(got.at[place_of(0, depth)], bulk_recv.at[k])

        def early(j):
            t = lax.rem(lax.rem(j, per_group), 4)

            @pl.when(jnp.logical_and(t != mine, lax.rem(t + 1, 4) != mine))
            def _():
                finish(j)

        loop(0, chunks, early)

    def late(i):
        hop = depth // 2 + jnp.where(lax.rem(i, 2) == 0, lax.div(i, 2), -lax.div(i + 1, 2))
        s = lax.rem(z + depth - hop, depth) * 4 + mine

        @pl.when(i < depth - 1)
        def _():
            wait_for(got.at[place_of(s)], bulk_recv.at[3 + i])

        q, u = lax.div(s, 8), lax.rem(s, 8)

        @pl.when(u > 0)
        def _():
            finish(q * per_group + u - 1)

        @pl.when(u < per_group)
        def _():
            finish(q * per_group + u)

    with jax.named_scope("late"):
        loop(0, depth - 1, lambda i: late(jnp.where(i == 0, depth - 1, i - 1)))
    with jax.named_scope("last"):
        late(depth - 2)

    with jax.named_scope("drain"):
        wait_for(got.at[place_of(0, peers)], bulk_send)


def solution(mesh):
    n_dp, n_mp = mesh.shape["dp"], mesh.shape["mp"]

    def per_device(activations, weight, thresholds):
        columns = weight.T
        cols, outs = columns.shape
        rows = outs // n_dp
        width = activations.shape[1]
        steps = 8
        dma = pltpu.SemaphoreType.DMA
        hbm, vmem = pl.BlockSpec(memory_space=pltpu.HBM), pl.BlockSpec(memory_space=pltpu.VMEM)
        return pl.pallas_call(
            functools.partial(kernel, n_dp, n_mp),
            out_shape=pltpu.VMEM((rows, width), jnp.bfloat16),
            in_specs=[hbm, hbm, hbm],
            out_specs=vmem,
            scratch_shapes=[
                pltpu.VMEM(activations.shape, jnp.bfloat16),
                pltpu.VMEM(columns.shape, jnp.bfloat16),
                pltpu.VMEM((n_dp * cols, rows), jnp.bfloat16),
                pltpu.VMEM((n_dp, 1, LANES), jnp.float32),
                pltpu.VMEM((n_dp, 1, LANES), jnp.float32),
                pltpu.VMEM((n_dp, 1, rows + LANES), jnp.float32),
                pltpu.VMEM((n_dp, 1, rows + LANES), jnp.float32),
                pltpu.VMEM((1, rows), jnp.float32),
                pltpu.VMEM((n_mp, 1, rows), jnp.float32),
                pltpu.VMEM((width // LANES, 1, LANES), jnp.float32),
                pltpu.VMEM((1, rows), jnp.float32),
                pltpu.VMEM((rows, LANES), jnp.float32),
                pltpu.VMEM((rows, LANES), jnp.float32),
                dma((steps,)), dma((3,)), dma, dma((n_dp // 4 + 2,)), dma((3,)), dma((3,)),
            ],
            compiler_params=pltpu.CompilerParams(collective_id=0, has_side_effects=True, vmem_limit_bytes=40 * 2**20),
        )(*(pltpu.with_memory_space_constraint(x, pltpu.HBM) for x in (activations, columns, thresholds.reshape(1, rows))))

    placed = (P("dp", "mp"), P(None, ("mp", "dp")), P("dp"))
    return jax.shard_map(per_device, mesh=mesh, in_specs=placed, out_specs=P("dp", "mp"), check_vma=False)
```

```python
import functools

import jax
import jax.numpy as jnp
from jax import lax
from jax.experimental import pallas as pl
from jax.experimental.pallas import tpu as pltpu
from jax.sharding import PartitionSpec as P

IN = 28672
LANES = 128
MESH = pl.DeviceIdType.MESH

gate_slope = 2.0
small_eps = 1e-06


NEAR = [(1, 3), (7, 3), (1, 2), (7, 2), (0, 2), (1, 0), (7, 0), (1, 1), (7, 1), (0, 0), (0, 1)]
FAR_HOPS = [4, 3, 5, 2, 6]
STAGES = [11, 22, 31]


def kernel(
    n_dp, n_mp, act_hbm, wt_hbm, thr_hbm, out_ref,
    act, wt, got, sq_send, sq_got, norm_all, norms, row_send, row_side, row_sum, row_z, tot_send, tot_got,
    limits, scale_a, scale_b,
    act_sem, local_sem, bulk_send, bulk_recv, small_send, small_recv, ring_sem,
):
    d, m = lax.axis_index("dp"), lax.axis_index("mp")
    cols, outs = wt_hbm.shape
    rows = outs // n_dp
    groups = n_dp // 8
    per_group = cols * 8 // LANES
    chunks = groups * per_group
    steps = act_sem.shape[0]
    tokens = act_hbm.shape[0] // steps
    depth = n_dp // 4
    peers = n_dp - 1

    z, high, core = lax.div(d, 4), lax.rem(lax.div(d, 2), 2), lax.rem(d, 2)
    sides = ((1 - high) * 2 + core, (1 - high) * 2 + 1 - core, high * 2 + 1 - core, high * 2 + core)
    mine = sides[3]
    blocks = NEAR + [(hop, side) for side in range(4) for hop in FAR_HOPS]
    assert sorted(blocks) == sorted((hop, side) for hop in range(depth) for side in range(4) if (hop, side) != (0, 3))
    SQUARES, ROW_SIDE, NORM_Z, ROW_Z, NORM_SIDE, TOTAL = range(6)

    def device(hop, side):
        return lax.rem(z + hop, depth) * 4 + sides[side]

    def mp_peer(i):
        return lax.rem(m + i, n_mp)

    def act_copy(i):
        span = pl.ds(pl.multiple_of(i * tokens, tokens), tokens)
        return pltpu.make_async_copy(act_hbm.at[span], act.at[span], act_sem.at[i])

    def block(i):
        return pl.ds(pl.multiple_of(i * rows, rows), rows)

    def place_of(i, n=1):
        return pl.ds(pl.multiple_of(i * cols, 16), n * cols)

    def remote(src, dst, ssem, rsem, to, row=None):
        pltpu.make_async_remote_copy(
            src_ref=src, dst_ref=dst, send_sem=ssem, recv_sem=rsem,
            device_id=(to, m) if row is None else (d, row), device_id_type=MESH,
        ).start()

    def bulk(stage):
        for hop, side in blocks[STAGES[stage - 1] if stage else 0:STAGES[stage]]:
            to = device(hop, side)
            i = 0 if (hop, side) in NEAR else 1 + side if side < 3 else 4 + FAR_HOPS.index(hop)
            remote(wt_hbm.at[:, block(to)], got.at[place_of(d)], bulk_send, bulk_recv.at[i], to)

    def to_plane(n, src, dst):
        for side in range(3):
            remote(src(sides[side]), dst, small_send.at[n], small_recv.at[n], device(0, side))

    def to_column(n, src, dst):
        for hop in (4, 3, 5, 2, 6, 1, 7):
            remote(src(lax.rem(z + hop, depth)), dst, small_send.at[n], small_recv.at[n], device(hop, 3))

    def wait_for(ref, sem):
        pltpu.make_async_copy(ref, ref, sem).wait()

    def loop(lo, hi, body):
        lax.fori_loop(lo, hi, lambda i, c: (body(i), c)[1], 0)

    with jax.named_scope("signal"):
        barrier = pltpu.get_barrier_semaphore()
        for hop in (1, depth - 1, 0):
            for side in range(4):
                if (hop, side) != (0, 3):
                    pl.semaphore_signal(barrier, inc=1, device_id=(device(hop, side), m), device_id_type=MESH)
        for i in range(1, n_mp):
            pl.semaphore_signal(barrier, inc=1, device_id=(d, mp_peer(i)), device_id_type=MESH)

    with jax.named_scope("local"):
        loop(0, steps, lambda i: act_copy(i).start())
        wt_local = pltpu.make_async_copy(wt_hbm, wt, local_sem.at[0])
        wt_local.start()
        own = pltpu.make_async_copy(wt_hbm.at[:, block(d)], got.at[place_of(d)], local_sem.at[1])
        own.start()
        limit_local = pltpu.make_async_copy(thr_hbm, limits, local_sem.at[2])
        limit_local.start()

    def ring_signal(r):
        for hop in (1, depth - 1):
            pl.semaphore_signal(ring_sem.at[r], inc=1, device_id=(device(hop, 3), m), device_id_type=MESH)

    with jax.named_scope("barrier"):
        pl.semaphore_wait(barrier, 11 + n_mp - 1)
    with jax.named_scope("near"):
        ring_signal(0)
        bulk(0)

    with jax.named_scope("squares"):
        def add_squares(i, sums):
            act_copy(i).wait()
            base = pl.multiple_of(i * tokens, tokens)
            out = []
            for j in range(chunks):
                x = act[pl.ds(base, tokens), j * LANES:(j + 1) * LANES].astype(jnp.float32)
                out.append(sums[j] + jnp.sum((x * x).reshape(tokens // 8, 8, LANES), axis=0))
            return tuple(out)

        sums = lax.fori_loop(0, steps, add_squares, tuple(jnp.zeros((8, LANES), jnp.float32) for _ in range(chunks)))
        sums = [jnp.sum(s, axis=0, keepdims=True) for s in sums]
        lane = lax.broadcasted_iota(jnp.int32, (1, LANES), 1)
        for q in range(groups):
            for u in range(8):
                shift = (LANES - cols) * u
                first = sums[per_group * q + max(u - 1, 0)]
                second = sums[per_group * q + min(u, per_group - 1)]
                if u:
                    first = pltpu.roll(first, shift, 1)
                    second = pltpu.roll(second, shift, 1)
                row = jnp.where(lane < shift, first, second)
                sq_send[8 * q + u] = jnp.where(lane < cols, row, 0.0)

    with jax.named_scope("ring0"):
        pl.semaphore_wait(ring_sem.at[0], 2)
        ring_signal(1)
    with jax.named_scope("ring1"):
        pl.semaphore_wait(ring_sem.at[1], 2)
        ring_signal(2)
    with jax.named_scope("ring2"):
        pl.semaphore_wait(ring_sem.at[2], 2)
    with jax.named_scope("issue"):
        for side in range(4):
            for hop in FAR_HOPS + [1, depth - 1, 0]:
                if (hop, side) != (0, 3):
                    to = device(hop, side)
                    remote(sq_send.at[to], sq_got.at[d], small_send.at[SQUARES], small_recv.at[SQUARES], to)
        bulk(1)
        sq_got[d] = sq_send[d]
        wt_local.wait()

    with jax.named_scope("wait_sq"):
        wait_for(sq_got.at[:peers], small_recv.at[SQUARES])

    with jax.named_scope("rowpart"):
        squares = jnp.sum(sq_got[...].reshape(n_dp // 8, 8, LANES), axis=0)
        squares = jnp.sum(squares, axis=0, keepdims=True)
        norm_lane = jnp.sqrt(squares)
        norm = jnp.broadcast_to(norm_lane, (LANES, LANES)).T[:cols]
        norm_all[mine, z] = norm_lane

        def row_part(r):
            for h in range(rows // LANES):
                w = wt[:, pl.ds(pl.multiple_of(r * rows + h * LANES, LANES), LANES)].astype(jnp.float32)
                part = jnp.sum((jnp.abs(w) * norm).reshape(cols // 8, 8, LANES), axis=0)
                row_send[lax.rem(r, 4), lax.div(r, 4), :, h * LANES:(h + 1) * LANES] = jnp.sum(part, axis=0, keepdims=True)

        loop(0, n_dp, row_part)
    with jax.named_scope("send_row"):
        to_plane(ROW_SIDE, lambda s: row_send.at[s], row_side.at[mine])
        to_column(NORM_Z, lambda p: norm_all.at[mine, z], norm_all.at[mine, z])
        row_side[mine] = row_send[mine]
    with jax.named_scope("wait_row"):
        wait_for(row_side.at[:3], small_recv.at[ROW_SIDE])
    with jax.named_scope("send_row2"):
        row_sum[...] = jnp.sum(row_side[...], axis=0)
        row_z[z] = row_sum[z]
        to_column(ROW_Z, lambda p: row_sum.at[p], row_z.at[z])
        bulk(2)
    with jax.named_scope("wait_norm"):
        wait_for(norm_all.at[0, :depth - 1], small_recv.at[NORM_Z])
        to_plane(NORM_SIDE, lambda s: norm_all.at[mine], norm_all.at[mine])
    with jax.named_scope("wait_row2"):
        wait_for(row_z.at[:depth - 1], small_recv.at[ROW_Z])
    with jax.named_scope("tot"):
        tot_send[...] = jnp.sum(row_z[...], axis=0)
        for i in range(1, n_mp):
            remote(tot_send, tot_got.at[m], small_send.at[TOTAL], small_recv.at[TOTAL], d, mp_peer(i))
        tot_got[m] = tot_send[...]
    with jax.named_scope("norms"):
        wait_for(norm_all.at[:3], small_recv.at[NORM_SIDE])
        for q in range(groups):
            for t in range(per_group):
                shift = (LANES - cols) * t
                first = norm_all[t % 4, 2 * q + t // 4]
                second = norm_all[(t + 1) % 4, 2 * q + (t + 1) // 4]
                first = pltpu.roll(first, LANES - shift, 1) if shift else first
                second = pltpu.roll(second, cols - shift, 1)
                norms[per_group * q + t] = jnp.where(lane < cols - shift, first, second)
        limit_local.wait()
        own.wait()
    with jax.named_scope("wait_tot"):
        wait_for(tot_got.at[:n_mp - 1], small_recv.at[TOTAL])

    with jax.named_scope("scale"):
        row_mean = jnp.sum(tot_got[...], axis=0) / IN + small_eps
        a = gate_slope / row_mean
        b = 0.5 - gate_slope * limits[...]
        for h in range(rows // LANES):
            part = slice(h * LANES, (h + 1) * LANES)
            scale_a[part] = jnp.broadcast_to(a[:, part], (LANES, LANES)).T
            scale_b[part] = jnp.broadcast_to(b[:, part], (LANES, LANES)).T
        for n, ref in (
            (SQUARES, sq_got.at[:peers]), (ROW_SIDE, row_side.at[:3]), (NORM_Z, norm_all.at[0, :depth - 1]),
            (ROW_Z, row_z.at[:depth - 1]), (NORM_SIDE, norm_all.at[:3]), (TOTAL, tot_got.at[:n_mp - 1]),
        ):
            wait_for(ref, small_send.at[n])

    def finish(j):
        span = pl.ds(pl.multiple_of(j * LANES, LANES), LANES)
        wide = got[span].T.astype(jnp.float32)
        scores = jnp.abs(wide) * norms[j]
        kept = jnp.clip(scores * scale_a[...] + scale_b[...], 0.0, 1.0)
        out_ref[:, span] = (wide * kept).astype(jnp.bfloat16)

    with jax.named_scope("early_wait"):
        wait_for(got.at[place_of(0, len(NEAR))], bulk_recv.at[0])
        for side in range(3):
            wait_for(got.at[place_of(0, len(FAR_HOPS))], bulk_recv.at[1 + side])

    def is_late(s):
        hop = lax.rem(z + depth - lax.div(s, 4), depth)
        return jnp.logical_and(lax.rem(s, 4) == mine, jnp.logical_and(hop > 1, hop < depth - 1))

    def early(j):
        s = lax.div(j, per_group) * 8 + lax.rem(j, per_group)

        @pl.when(jnp.logical_not(jnp.logical_or(is_late(s), is_late(s + 1))))
        def _():
            finish(j)

    with jax.named_scope("early"):
        loop(0, chunks, early)

    for k, hop in enumerate(FAR_HOPS):
        with jax.named_scope("late%d" % k):
            wait_for(got.at[place_of(0)], bulk_recv.at[4 + k])
            s = lax.rem(z + depth - hop, depth) * 4 + mine
            q, u = lax.div(s, 8), lax.rem(s, 8)
            lo, hi = jnp.where(u > 0, u - 1, 0), jnp.where(u < per_group, u + 1, per_group)
            loop(q * per_group + lo, q * per_group + hi, finish)

    with jax.named_scope("drain"):
        wait_for(got.at[place_of(0, peers)], bulk_send)


def solution(mesh):
    n_dp, n_mp = mesh.shape["dp"], mesh.shape["mp"]

    def per_device(activations, weight, thresholds):
        columns = weight.T
        cols, outs = columns.shape
        rows = outs // n_dp
        width = activations.shape[1]
        steps = 8
        depth = n_dp // 4
        dma = pltpu.SemaphoreType.DMA

        def f32(*shape):
            return pltpu.VMEM(shape, jnp.float32)

        hbm, vmem = pl.BlockSpec(memory_space=pltpu.HBM), pl.BlockSpec(memory_space=pltpu.VMEM)
        return pl.pallas_call(
            functools.partial(kernel, n_dp, n_mp),
            out_shape=pltpu.VMEM((rows, width), jnp.bfloat16),
            in_specs=[hbm, hbm, hbm],
            out_specs=vmem,
            scratch_shapes=[
                pltpu.VMEM(activations.shape, jnp.bfloat16),
                pltpu.VMEM(columns.shape, jnp.bfloat16),
                pltpu.VMEM((n_dp * cols, rows), jnp.bfloat16),
                f32(n_dp, 1, LANES), f32(n_dp, 1, LANES),
                f32(4, depth, 1, LANES), f32(width // LANES, 1, LANES),
                f32(4, depth, 1, rows), f32(4, depth, 1, rows), f32(depth, 1, rows), f32(depth, 1, rows),
                f32(1, rows), f32(n_mp, 1, rows),
                f32(1, rows), f32(rows, LANES), f32(rows, LANES),
                dma((steps,)), dma((3,)), dma, dma((4 + len(FAR_HOPS),)), dma((6,)), dma((6,)), pltpu.SemaphoreType.REGULAR((3,)),
            ],
            compiler_params=pltpu.CompilerParams(collective_id=0, has_side_effects=True, vmem_limit_bytes=40 * 2**20),
        )(*(pltpu.with_memory_space_constraint(x, pltpu.HBM) for x in (activations, columns, thresholds.reshape(1, rows))))

    placed = (P("dp", "mp"), P(None, ("mp", "dp")), P("dp"))
    return jax.shard_map(per_device, mesh=mesh, in_specs=placed, out_specs=P("dp", "mp"), check_vma=False)
```

```python
import functools

import jax
import jax.numpy as jnp
from jax import lax
from jax.experimental import pallas as pl
from jax.experimental.pallas import tpu as pltpu
from jax.sharding import PartitionSpec as P

IN = 28672
LANES = 128
MESH = pl.DeviceIdType.MESH

gate_slope = 2.0
small_eps = 1e-06


SAME = [(1, 3), (7, 3), (1, 2), (7, 2), (0, 2)]
CROSS = [(1, 0), (7, 0), (1, 1), (7, 1), (0, 0), (0, 1)]
NEAR = SAME + CROSS
FAR_HOPS = [4, 3, 5, 2, 6]
SWEEPS = [0, 2, 1, 3]
AHEAD = [(4, 2), (3, 2), (5, 2)]
ORDER = NEAR + AHEAD + [(hop, side) for side in SWEEPS for hop in FAR_HOPS if (hop, side) not in AHEAD]
STAGES = [5, 11, 22, 31]
SPLIT = 4


def kernel(
    n_dp, n_mp, act_hbm, wt_hbm, thr_hbm, out_ref,
    act, wt, got, sq_send, sq_got, norm_all, norms, row_send, row_side, row_sum, row_z, tot_send, tot_got,
    limits, scale_a, scale_b, half,
    act_sem, local_sem, bulk_send, bulk_recv, small_send, small_recv, ring_sem, cross_sem, row_sem,
):
    d, m = lax.axis_index("dp"), lax.axis_index("mp")
    cols, outs = wt_hbm.shape
    rows = outs // n_dp
    groups = n_dp // 8
    per_group = cols * 8 // LANES
    chunks = groups * per_group
    steps = act_sem.shape[0]
    tokens = act_hbm.shape[0] // steps
    depth = n_dp // 4
    peers = n_dp - 1

    z, high, core = lax.div(d, 4), lax.rem(lax.div(d, 2), 2), lax.rem(d, 2)
    sides = ((1 - high) * 2 + core, (1 - high) * 2 + 1 - core, high * 2 + 1 - core, high * 2 + core)
    mine = sides[3]
    assert sorted(ORDER) == sorted((hop, side) for hop in range(depth) for side in range(4) if (hop, side) != (0, 3))
    SQUARES, ROW_SIDE, NORM_Z, ROW_Z, NORM_SIDE, TOTAL = range(6)

    def device(hop, side):
        return lax.rem(z + hop, depth) * 4 + sides[side]

    def mp_peer(i):
        return lax.rem(m + i, n_mp)

    def act_copy(i):
        span = pl.ds(pl.multiple_of(i * tokens, tokens), tokens)
        return pltpu.make_async_copy(act_hbm.at[span], act.at[span], act_sem.at[i])

    def block(i):
        return pl.ds(pl.multiple_of(i * rows, rows), rows)

    def place_of(i, n=1):
        return pl.ds(pl.multiple_of(i * cols, 16), n * cols)

    def remote(src, dst, ssem, rsem, to, row=None):
        pltpu.make_async_remote_copy(
            src_ref=src, dst_ref=dst, send_sem=ssem, recv_sem=rsem,
            device_id=(to, m) if row is None else (d, row), device_id_type=MESH,
        ).start()

    def bulk(stage):
        for hop, side in ORDER[STAGES[stage - 1] if stage else 0:STAGES[stage]]:
            to = device(hop, side)
            i = 0 if (hop, side) in NEAR else 1 + side if side < 3 else 4 + FAR_HOPS.index(hop)
            remote(wt_hbm.at[:, block(to)], got.at[place_of(d)], bulk_send, bulk_recv.at[i], to)

    def to_plane(n, src, dst):
        for side in range(3):
            remote(src(sides[side]), dst, small_send.at[n], small_recv.at[n], device(0, side))

    def to_column(n, src, dst):
        for hop in (4, 3, 5, 2, 6, 1, 7):
            remote(src(lax.rem(z + hop, depth)), dst, small_send.at[n], small_recv.at[n], device(hop, 3))

    def wait_for(ref, sem):
        pltpu.make_async_copy(ref, ref, sem).wait()

    def loop(lo, hi, body):
        lax.fori_loop(lo, hi, lambda i, c: (body(i), c)[1], 0)

    upper, leader = high == 1, m == n_mp - 1

    def signal(sem, to, row=None):
        pl.semaphore_signal(sem, inc=1, device_id=(to, m) if row is None else (d, row), device_id_type=MESH)

    with jax.named_scope("signal"):
        barrier = pltpu.get_barrier_semaphore()
        for hop, side in SAME:
            signal(barrier, device(hop, side))

        @pl.when(jnp.logical_not(upper))
        def _():
            for hop, side in CROSS:
                signal(barrier, device(hop, side))

        @pl.when(jnp.logical_not(leader))
        def _():
            signal(barrier, d, n_mp - 1)

    with jax.named_scope("local"):
        loop(0, steps, lambda i: act_copy(i).start())
        wt_local = pltpu.make_async_copy(wt_hbm, wt, local_sem.at[0])
        wt_local.start()
        own = pltpu.make_async_copy(wt_hbm.at[:, block(d)], got.at[place_of(d)], local_sem.at[1])
        own.start()
        limit_local = pltpu.make_async_copy(thr_hbm, limits, local_sem.at[2])
        limit_local.start()

    def ring_signal(r):
        for hop in (1, depth - 1):
            signal(ring_sem.at[r], device(hop, 3))

    with jax.named_scope("barrier"):
        pl.semaphore_wait(barrier, len(SAME) + len(CROSS) * upper.astype(jnp.int32) + (n_mp - 1) * leader.astype(jnp.int32))
    with jax.named_scope("near"):
        ring_signal(0)
        bulk(0)

        @pl.when(upper)
        def _():
            signal(cross_sem.at[0], device(0, 0))

        @pl.when(leader)
        def _():
            for i in range(1, n_mp):
                signal(row_sem, d, mp_peer(i))

    with jax.named_scope("squares"):
        def add_squares(i, sums):
            act_copy(i).wait()
            base = pl.multiple_of(i * tokens, tokens)
            out = []
            for j in range(chunks):
                x = act[pl.ds(base, tokens), j * LANES:(j + 1) * LANES].astype(jnp.float32)
                out.append(sums[j] + jnp.sum((x * x).reshape(tokens // 8, 8, LANES), axis=0))
            return tuple(out)

        sums = lax.fori_loop(0, SPLIT, add_squares, tuple(jnp.zeros((8, LANES), jnp.float32) for _ in range(chunks)))
        for j in range(chunks):
            half[j] = sums[j]
    with jax.named_scope("ring0"):
        pl.semaphore_wait(ring_sem.at[0], 2)
        ring_signal(1)

        @pl.when(jnp.logical_not(upper))
        def _():
            pl.semaphore_wait(cross_sem.at[0], 1)

        bulk(1)
    with jax.named_scope("squares2"):
        sums = lax.fori_loop(SPLIT, steps, add_squares, tuple(half[j] for j in range(chunks)))
        sums = [jnp.sum(s, axis=0, keepdims=True) for s in sums]
        lane = lax.broadcasted_iota(jnp.int32, (1, LANES), 1)
        for q in range(groups):
            for u in range(8):
                shift = (LANES - cols) * u
                first = sums[per_group * q + max(u - 1, 0)]
                second = sums[per_group * q + min(u, per_group - 1)]
                if u:
                    first = pltpu.roll(first, shift, 1)
                    second = pltpu.roll(second, shift, 1)
                row = jnp.where(lane < shift, first, second)
                sq_send[8 * q + u] = jnp.where(lane < cols, row, 0.0)

    def send_squares(sides_of):
        for side in sides_of:
            for hop in FAR_HOPS + [1, depth - 1, 0]:
                if (hop, side) != (0, 3):
                    to = device(hop, side)
                    remote(sq_send.at[to], sq_got.at[d], small_send.at[SQUARES], small_recv.at[SQUARES], to)

    with jax.named_scope("ring1"):
        pl.semaphore_wait(ring_sem.at[1], 2)
        ring_signal(2)
    with jax.named_scope("ring2"):
        pl.semaphore_wait(ring_sem.at[2], 2)
        signal(cross_sem.at[1], device(0, 0))
        send_squares((2, 3))
    with jax.named_scope("cross"):
        pl.semaphore_wait(cross_sem.at[1], 1)
    with jax.named_scope("issue"):
        send_squares((0, 1))
        bulk(2)
        sq_got[d] = sq_send[d]
        wt_local.wait()

    with jax.named_scope("wait_sq"):
        wait_for(sq_got.at[:peers], small_recv.at[SQUARES])

    with jax.named_scope("rowpart"):
        squares = jnp.sum(sq_got[...].reshape(n_dp // 8, 8, LANES), axis=0)
        squares = jnp.sum(squares, axis=0, keepdims=True)
        norm_lane = jnp.sqrt(squares)
        norm = jnp.broadcast_to(norm_lane, (LANES, LANES)).T[:cols]
        norm_all[mine, z] = norm_lane

        def row_part(r):
            for h in range(rows // LANES):
                w = wt[:, pl.ds(pl.multiple_of(r * rows + h * LANES, LANES), LANES)].astype(jnp.float32)
                part = jnp.sum((jnp.abs(w) * norm).reshape(cols // 8, 8, LANES), axis=0)
                row_send[lax.rem(r, 4), lax.div(r, 4), :, h * LANES:(h + 1) * LANES] = jnp.sum(part, axis=0, keepdims=True)

        loop(0, n_dp, row_part)
    with jax.named_scope("send_row"):
        to_plane(ROW_SIDE, lambda s: row_send.at[s], row_side.at[mine])
        to_column(NORM_Z, lambda p: norm_all.at[mine, z], norm_all.at[mine, z])
        row_side[mine] = row_send[mine]
    with jax.named_scope("wait_row"):
        wait_for(row_side.at[:3], small_recv.at[ROW_SIDE])
    with jax.named_scope("send_row2"):
        row_sum[...] = jnp.sum(row_side[...], axis=0)
        row_z[z] = row_sum[z]
        to_column(ROW_Z, lambda p: row_sum.at[p], row_z.at[z])
        bulk(3)
    with jax.named_scope("wait_norm"):
        wait_for(norm_all.at[0, :depth - 1], small_recv.at[NORM_Z])
        to_plane(NORM_SIDE, lambda s: norm_all.at[mine], norm_all.at[mine])
    with jax.named_scope("wait_row2"):
        wait_for(row_z.at[:depth - 1], small_recv.at[ROW_Z])
    with jax.named_scope("tot"):
        tot_send[...] = jnp.sum(row_z[...], axis=0)

        @pl.when(jnp.logical_not(leader))
        def _():
            pl.semaphore_wait(row_sem, 1)

        for i in range(1, n_mp):
            remote(tot_send, tot_got.at[m], small_send.at[TOTAL], small_recv.at[TOTAL], d, mp_peer(i))
        tot_got[m] = tot_send[...]
    with jax.named_scope("norms"):
        wait_for(norm_all.at[:3], small_recv.at[NORM_SIDE])
        for q in range(groups):
            for t in range(per_group):
                shift = (LANES - cols) * t
                first = norm_all[t % 4, 2 * q + t // 4]
                second = norm_all[(t + 1) % 4, 2 * q + (t + 1) // 4]
                first = pltpu.roll(first, LANES - shift, 1) if shift else first
                second = pltpu.roll(second, cols - shift, 1)
                norms[per_group * q + t] = jnp.where(lane < cols - shift, first, second)
        limit_local.wait()
        own.wait()
    with jax.named_scope("wait_tot"):
        wait_for(tot_got.at[:n_mp - 1], small_recv.at[TOTAL])

    with jax.named_scope("scale"):
        row_mean = jnp.sum(tot_got[...], axis=0) / IN + small_eps
        a = gate_slope / row_mean
        b = 0.5 - gate_slope * limits[...]
        for h in range(rows // LANES):
            part = slice(h * LANES, (h + 1) * LANES)
            scale_a[part] = jnp.broadcast_to(a[:, part], (LANES, LANES)).T
            scale_b[part] = jnp.broadcast_to(b[:, part], (LANES, LANES)).T
        for n, ref in (
            (SQUARES, sq_got.at[:peers]), (ROW_SIDE, row_side.at[:3]), (NORM_Z, norm_all.at[0, :depth - 1]),
            (ROW_Z, row_z.at[:depth - 1]), (NORM_SIDE, norm_all.at[:3]), (TOTAL, tot_got.at[:n_mp - 1]),
        ):
            wait_for(ref, small_send.at[n])

    def finish(j):
        span = pl.ds(pl.multiple_of(j * LANES, LANES), LANES)
        wide = got[span].T.astype(jnp.float32)
        scores = jnp.abs(wide) * norms[j]
        kept = jnp.clip(scores * scale_a[...] + scale_b[...], 0.0, 1.0)
        out_ref[:, span] = (wide * kept).astype(jnp.bfloat16)

    with jax.named_scope("early_wait"):
        wait_for(got.at[place_of(0, len(NEAR))], bulk_recv.at[0])
        for side in range(3):
            wait_for(got.at[place_of(0, len(FAR_HOPS))], bulk_recv.at[1 + side])

    def is_late(s):
        hop = lax.rem(z + depth - lax.div(s, 4), depth)
        return jnp.logical_and(lax.rem(s, 4) == mine, jnp.logical_and(hop > 1, hop < depth - 1))

    def early(j):
        s = lax.div(j, per_group) * 8 + lax.rem(j, per_group)

        @pl.when(jnp.logical_not(jnp.logical_or(is_late(s), is_late(s + 1))))
        def _():
            finish(j)

    with jax.named_scope("early"):
        loop(0, chunks, early)

    for k, hop in enumerate(FAR_HOPS):
        with jax.named_scope("late%d" % k):
            wait_for(got.at[place_of(0)], bulk_recv.at[4 + k])
            s = lax.rem(z + depth - hop, depth) * 4 + mine
            q, u = lax.div(s, 8), lax.rem(s, 8)
            lo, hi = jnp.where(u > 0, u - 1, 0), jnp.where(u < per_group, u + 1, per_group)
            loop(q * per_group + lo, q * per_group + hi, finish)

    with jax.named_scope("drain"):
        wait_for(got.at[place_of(0, peers)], bulk_send)


def solution(mesh):
    n_dp, n_mp = mesh.shape["dp"], mesh.shape["mp"]

    def per_device(activations, weight, thresholds):
        columns = weight.T
        cols, outs = columns.shape
        rows = outs // n_dp
        width = activations.shape[1]
        steps = 8
        depth = n_dp // 4
        dma, regular = pltpu.SemaphoreType.DMA, pltpu.SemaphoreType.REGULAR

        def f32(*shape):
            return pltpu.VMEM(shape, jnp.float32)

        hbm, vmem = pl.BlockSpec(memory_space=pltpu.HBM), pl.BlockSpec(memory_space=pltpu.VMEM)
        return pl.pallas_call(
            functools.partial(kernel, n_dp, n_mp),
            out_shape=pltpu.VMEM((rows, width), jnp.bfloat16),
            in_specs=[hbm, hbm, hbm],
            out_specs=vmem,
            scratch_shapes=[
                pltpu.VMEM(activations.shape, jnp.bfloat16),
                pltpu.VMEM(columns.shape, jnp.bfloat16),
                pltpu.VMEM((n_dp * cols, rows), jnp.bfloat16),
                f32(n_dp, 1, LANES), f32(n_dp, 1, LANES),
                f32(4, depth, 1, LANES), f32(width // LANES, 1, LANES),
                f32(4, depth, 1, rows), f32(4, depth, 1, rows), f32(depth, 1, rows), f32(depth, 1, rows),
                f32(1, rows), f32(n_mp, 1, rows),
                f32(1, rows), f32(rows, LANES), f32(rows, LANES), f32(width // LANES, 8, LANES),
                dma((steps,)), dma((3,)), dma, dma((4 + len(FAR_HOPS),)), dma((6,)), dma((6,)), regular((3,)), regular((2,)), regular,
            ],
            compiler_params=pltpu.CompilerParams(collective_id=0, has_side_effects=True, vmem_limit_bytes=40 * 2**20),
        )(*(pltpu.with_memory_space_constraint(x, pltpu.HBM) for x in (activations, columns, thresholds.reshape(1, rows))))

    placed = (P("dp", "mp"), P(None, ("mp", "dp")), P("dp"))
    return jax.shard_map(per_device, mesh=mesh, in_specs=placed, out_specs=P("dp", "mp"), check_vma=False)
```

```python
import functools

import jax
import jax.numpy as jnp
from jax import lax
from jax.experimental import pallas as pl
from jax.experimental.pallas import tpu as pltpu
from jax.sharding import PartitionSpec as P

IN = 28672
LANES = 128
MESH = pl.DeviceIdType.MESH

gate_slope = 2.0
small_eps = 1e-06


SAME = [(1, 3), (7, 3), (1, 2), (7, 2), (0, 2)]
CROSS = [(1, 0), (7, 0), (1, 1), (7, 1), (0, 0), (0, 1)]
NEAR = SAME + CROSS
FAR_HOPS = [4, 3, 5, 2, 6]
SWEEPS = [0, 2, 1, 3]
ORDER = NEAR + [(hop, side) for side in SWEEPS for hop in FAR_HOPS]
STAGES = [5, 11, 22, 31]
SPLIT = 0


def kernel(
    n_dp, n_mp, act_hbm, wt_hbm, thr_hbm, out_ref,
    act, wt, got, sq_send, sq_got, norm_all, norms, row_send, row_side, row_sum, row_z, tot_send, tot_got,
    limits, scale_a, scale_b, half,
    act_sem, local_sem, bulk_send, bulk_recv, small_send, small_recv, ring_sem, cross_sem, row_sem,
):
    d, m = lax.axis_index("dp"), lax.axis_index("mp")
    cols, outs = wt_hbm.shape
    rows = outs // n_dp
    groups = n_dp // 8
    per_group = cols * 8 // LANES
    chunks = groups * per_group
    steps = act_sem.shape[0]
    tokens = act_hbm.shape[0] // steps
    depth = n_dp // 4
    peers = n_dp - 1

    z, high, core = lax.div(d, 4), lax.rem(lax.div(d, 2), 2), lax.rem(d, 2)
    sides = ((1 - high) * 2 + core, (1 - high) * 2 + 1 - core, high * 2 + 1 - core, high * 2 + core)
    mine = sides[3]
    assert sorted(ORDER) == sorted((hop, side) for hop in range(depth) for side in range(4) if (hop, side) != (0, 3))
    SQUARES, ROW_SIDE, NORM_Z, ROW_Z, NORM_SIDE, TOTAL = range(6)

    def device(hop, side):
        return lax.rem(z + hop, depth) * 4 + sides[side]

    def mp_peer(i):
        return lax.rem(m + i, n_mp)

    def act_copy(i):
        span = pl.ds(pl.multiple_of(i * tokens, tokens), tokens)
        return pltpu.make_async_copy(act_hbm.at[span], act.at[span], act_sem.at[i])

    def block(i):
        return pl.ds(pl.multiple_of(i * rows, rows), rows)

    def place_of(i, n=1):
        return pl.ds(pl.multiple_of(i * cols, 16), n * cols)

    def remote(src, dst, ssem, rsem, to, row=None):
        pltpu.make_async_remote_copy(
            src_ref=src, dst_ref=dst, send_sem=ssem, recv_sem=rsem,
            device_id=(to, m) if row is None else (d, row), device_id_type=MESH,
        ).start()

    def bulk(stage):
        for hop, side in ORDER[STAGES[stage - 1] if stage else 0:STAGES[stage]]:
            to = device(hop, side)
            i = 0 if (hop, side) in NEAR else 1 + side if side < 3 else 4 + FAR_HOPS.index(hop)
            remote((wt_hbm if stage < 2 else wt).at[:, block(to)], got.at[place_of(d)], bulk_send, bulk_recv.at[i], to)

    def to_plane(n, src, dst):
        for side in range(3):
            remote(src(sides[side]), dst, small_send.at[n], small_recv.at[n], device(0, side))

    def to_column(n, src, dst):
        for hop in (4, 3, 5, 2, 6, 1, 7):
            remote(src(lax.rem(z + hop, depth)), dst, small_send.at[n], small_recv.at[n], device(hop, 3))

    def wait_for(ref, sem):
        pltpu.make_async_copy(ref, ref, sem).wait()

    def loop(lo, hi, body):
        lax.fori_loop(lo, hi, lambda i, c: (body(i), c)[1], 0)

    upper, leader = high == 1, m == n_mp - 1

    def signal(sem, to, row=None):
        pl.semaphore_signal(sem, inc=1, device_id=(to, m) if row is None else (d, row), device_id_type=MESH)

    with jax.named_scope("signal"):
        barrier = pltpu.get_barrier_semaphore()
        for hop, side in SAME:
            signal(barrier, device(hop, side))

        @pl.when(jnp.logical_not(upper))
        def _():
            for hop, side in CROSS:
                signal(barrier, device(hop, side))

        @pl.when(jnp.logical_not(leader))
        def _():
            signal(barrier, d, n_mp - 1)

    with jax.named_scope("local"):
        loop(0, steps, lambda i: act_copy(i).start())
        wt_local = pltpu.make_async_copy(wt_hbm, wt, local_sem.at[0])
        wt_local.start()
        own = pltpu.make_async_copy(wt_hbm.at[:, block(d)], got.at[place_of(d)], local_sem.at[1])
        own.start()
        limit_local = pltpu.make_async_copy(thr_hbm, limits, local_sem.at[2])
        limit_local.start()

    def ring_signal(r):
        for hop in (1, depth - 1):
            signal(ring_sem.at[r], device(hop, 3))

    with jax.named_scope("barrier"):
        pl.semaphore_wait(barrier, len(SAME) + len(CROSS) * upper.astype(jnp.int32) + (n_mp - 1) * leader.astype(jnp.int32))
    with jax.named_scope("near"):
        ring_signal(0)
        bulk(0)

        @pl.when(upper)
        def _():
            signal(cross_sem.at[0], device(0, 0))

        @pl.when(leader)
        def _():
            for i in range(1, n_mp):
                signal(row_sem, d, mp_peer(i))

    with jax.named_scope("squares"):
        def add_squares(i, sums):
            act_copy(i).wait()
            base = pl.multiple_of(i * tokens, tokens)
            out = []
            for j in range(chunks):
                x = act[pl.ds(base, tokens), j * LANES:(j + 1) * LANES].astype(jnp.float32)
                out.append(sums[j] + jnp.sum((x * x).reshape(tokens // 8, 8, LANES), axis=0))
            return tuple(out)

        sums = lax.fori_loop(0, SPLIT, add_squares, tuple(jnp.zeros((8, LANES), jnp.float32) for _ in range(chunks)))
        for j in range(chunks):
            half[j] = sums[j]
    with jax.named_scope("ring0"):
        pl.semaphore_wait(ring_sem.at[0], 2)
        ring_signal(1)

        @pl.when(jnp.logical_not(upper))
        def _():
            pl.semaphore_wait(cross_sem.at[0], 1)

        bulk(1)
    with jax.named_scope("squares2"):
        sums = lax.fori_loop(SPLIT, steps, add_squares, tuple(half[j] for j in range(chunks)))
        sums = [jnp.sum(s, axis=0, keepdims=True) for s in sums]
        lane = lax.broadcasted_iota(jnp.int32, (1, LANES), 1)
        for q in range(groups):
            for u in range(8):
                shift = (LANES - cols) * u
                first = sums[per_group * q + max(u - 1, 0)]
                second = sums[per_group * q + min(u, per_group - 1)]
                if u:
                    first = pltpu.roll(first, shift, 1)
                    second = pltpu.roll(second, shift, 1)
                row = jnp.where(lane < shift, first, second)
                sq_send[8 * q + u] = jnp.where(lane < cols, row, 0.0)

    def send_squares(sides_of):
        for side in sides_of:
            for hop in FAR_HOPS + [1, depth - 1, 0]:
                if (hop, side) != (0, 3):
                    to = device(hop, side)
                    remote(sq_send.at[to], sq_got.at[d], small_send.at[SQUARES], small_recv.at[SQUARES], to)

    with jax.named_scope("ring1"):
        pl.semaphore_wait(ring_sem.at[1], 2)
        ring_signal(2)
    with jax.named_scope("ring2"):
        pl.semaphore_wait(ring_sem.at[2], 2)
        signal(cross_sem.at[1], device(0, 0))
        send_squares((2, 3))
    with jax.named_scope("cross"):
        pl.semaphore_wait(cross_sem.at[1], 1)
    with jax.named_scope("issue"):
        send_squares((0, 1))
        wt_local.wait()
        bulk(2)
        sq_got[d] = sq_send[d]

    with jax.named_scope("wait_sq"):
        wait_for(sq_got.at[:peers], small_recv.at[SQUARES])

    with jax.named_scope("rowpart"):
        squares = jnp.sum(sq_got[...].reshape(n_dp // 8, 8, LANES), axis=0)
        squares = jnp.sum(squares, axis=0, keepdims=True)
        norm_lane = jnp.sqrt(squares)
        norm = jnp.broadcast_to(norm_lane, (LANES, LANES)).T[:cols]
        norm_all[mine, z] = norm_lane

        def row_part(r):
            for h in range(rows // LANES):
                w = wt[:, pl.ds(pl.multiple_of(r * rows + h * LANES, LANES), LANES)].astype(jnp.float32)
                part = jnp.sum((jnp.abs(w) * norm).reshape(cols // 8, 8, LANES), axis=0)
                row_send[lax.rem(r, 4), lax.div(r, 4), :, h * LANES:(h + 1) * LANES] = jnp.sum(part, axis=0, keepdims=True)

        loop(0, n_dp, row_part)
    with jax.named_scope("send_row"):
        to_plane(ROW_SIDE, lambda s: row_send.at[s], row_side.at[mine])
        to_column(NORM_Z, lambda p: norm_all.at[mine, z], norm_all.at[mine, z])
        row_side[mine] = row_send[mine]
    with jax.named_scope("wait_row"):
        wait_for(row_side.at[:3], small_recv.at[ROW_SIDE])
    with jax.named_scope("send_row2"):
        row_sum[...] = jnp.sum(row_side[...], axis=0)
        row_z[z] = row_sum[z]
        to_column(ROW_Z, lambda p: row_sum.at[p], row_z.at[z])
        bulk(3)
    with jax.named_scope("wait_norm"):
        wait_for(norm_all.at[0, :depth - 1], small_recv.at[NORM_Z])
        to_plane(NORM_SIDE, lambda s: norm_all.at[mine], norm_all.at[mine])
    with jax.named_scope("wait_row2"):
        wait_for(row_z.at[:depth - 1], small_recv.at[ROW_Z])
    with jax.named_scope("tot"):
        tot_send[...] = jnp.sum(row_z[...], axis=0)

        @pl.when(jnp.logical_not(leader))
        def _():
            pl.semaphore_wait(row_sem, 1)

        for i in range(1, n_mp):
            remote(tot_send, tot_got.at[m], small_send.at[TOTAL], small_recv.at[TOTAL], d, mp_peer(i))
        tot_got[m] = tot_send[...]
    with jax.named_scope("norms"):
        wait_for(norm_all.at[:3], small_recv.at[NORM_SIDE])
        for q in range(groups):
            for t in range(per_group):
                shift = (LANES - cols) * t
                first = norm_all[t % 4, 2 * q + t // 4]
                second = norm_all[(t + 1) % 4, 2 * q + (t + 1) // 4]
                first = pltpu.roll(first, LANES - shift, 1) if shift else first
                second = pltpu.roll(second, cols - shift, 1)
                norms[per_group * q + t] = jnp.where(lane < cols - shift, first, second)
        limit_local.wait()
        own.wait()
    with jax.named_scope("wait_tot"):
        wait_for(tot_got.at[:n_mp - 1], small_recv.at[TOTAL])

    with jax.named_scope("scale"):
        row_mean = jnp.sum(tot_got[...], axis=0) / IN + small_eps
        a = gate_slope / row_mean
        b = 0.5 - gate_slope * limits[...]
        for h in range(rows // LANES):
            part = slice(h * LANES, (h + 1) * LANES)
            scale_a[part] = jnp.broadcast_to(a[:, part], (LANES, LANES)).T
            scale_b[part] = jnp.broadcast_to(b[:, part], (LANES, LANES)).T
        for n, ref in (
            (SQUARES, sq_got.at[:peers]), (ROW_SIDE, row_side.at[:3]), (NORM_Z, norm_all.at[0, :depth - 1]),
            (ROW_Z, row_z.at[:depth - 1]), (NORM_SIDE, norm_all.at[:3]), (TOTAL, tot_got.at[:n_mp - 1]),
        ):
            wait_for(ref, small_send.at[n])

    def finish(j):
        span = pl.ds(pl.multiple_of(j * LANES, LANES), LANES)
        wide = got[span].T.astype(jnp.float32)
        scores = jnp.abs(wide) * norms[j]
        kept = jnp.clip(scores * scale_a[...] + scale_b[...], 0.0, 1.0)
        out_ref[:, span] = (wide * kept).astype(jnp.bfloat16)

    with jax.named_scope("early_wait"):
        wait_for(got.at[place_of(0, len(NEAR))], bulk_recv.at[0])
        for side in range(3):
            wait_for(got.at[place_of(0, len(FAR_HOPS))], bulk_recv.at[1 + side])

    def is_late(s):
        hop = lax.rem(z + depth - lax.div(s, 4), depth)
        return jnp.logical_and(lax.rem(s, 4) == mine, jnp.logical_and(hop > 1, hop < depth - 1))

    def early(j):
        s = lax.div(j, per_group) * 8 + lax.rem(j, per_group)

        @pl.when(jnp.logical_not(jnp.logical_or(is_late(s), is_late(s + 1))))
        def _():
            finish(j)

    with jax.named_scope("early"):
        loop(0, chunks, early)

    for k, hop in enumerate(FAR_HOPS):
        with jax.named_scope("late%d" % k):
            wait_for(got.at[place_of(0)], bulk_recv.at[4 + k])
            s = lax.rem(z + depth - hop, depth) * 4 + mine
            q, u = lax.div(s, 8), lax.rem(s, 8)
            lo, hi = jnp.where(u > 0, u - 1, 0), jnp.where(u < per_group, u + 1, per_group)
            loop(q * per_group + lo, q * per_group + hi, finish)

    with jax.named_scope("drain"):
        wait_for(got.at[place_of(0, peers)], bulk_send)


def solution(mesh):
    n_dp, n_mp = mesh.shape["dp"], mesh.shape["mp"]

    def per_device(activations, weight, thresholds):
        columns = weight.T
        cols, outs = columns.shape
        rows = outs // n_dp
        width = activations.shape[1]
        steps = 8
        depth = n_dp // 4
        dma, regular = pltpu.SemaphoreType.DMA, pltpu.SemaphoreType.REGULAR

        def f32(*shape):
            return pltpu.VMEM(shape, jnp.float32)

        hbm, vmem = pl.BlockSpec(memory_space=pltpu.HBM), pl.BlockSpec(memory_space=pltpu.VMEM)
        return pl.pallas_call(
            functools.partial(kernel, n_dp, n_mp),
            out_shape=pltpu.VMEM((rows, width), jnp.bfloat16),
            in_specs=[hbm, hbm, hbm],
            out_specs=vmem,
            scratch_shapes=[
                pltpu.VMEM(activations.shape, jnp.bfloat16),
                pltpu.VMEM(columns.shape, jnp.bfloat16),
                pltpu.VMEM((n_dp * cols, rows), jnp.bfloat16),
                f32(n_dp, 1, LANES), f32(n_dp, 1, LANES),
                f32(4, depth, 1, LANES), f32(width // LANES, 1, LANES),
                f32(4, depth, 1, rows), f32(4, depth, 1, rows), f32(depth, 1, rows), f32(depth, 1, rows),
                f32(1, rows), f32(n_mp, 1, rows),
                f32(1, rows), f32(rows, LANES), f32(rows, LANES), f32(width // LANES, 8, LANES),
                dma((steps,)), dma((3,)), dma, dma((4 + len(FAR_HOPS),)), dma((6,)), dma((6,)), regular((3,)), regular((2,)), regular,
            ],
            compiler_params=pltpu.CompilerParams(collective_id=0, has_side_effects=True, vmem_limit_bytes=40 * 2**20),
        )(*(pltpu.with_memory_space_constraint(x, pltpu.HBM) for x in (activations, columns, thresholds.reshape(1, rows))))

    placed = (P("dp", "mp"), P(None, ("mp", "dp")), P("dp"))
    return jax.shard_map(per_device, mesh=mesh, in_specs=placed, out_specs=P("dp", "mp"), check_vma=False)
```

```python
import functools

import jax
import jax.numpy as jnp
from jax import lax
from jax.experimental import pallas as pl
from jax.experimental.pallas import tpu as pltpu
from jax.sharding import PartitionSpec as P

IN = 28672
LANES = 128
MESH = pl.DeviceIdType.MESH

gate_slope = 2.0
small_eps = 1e-06


SAME = [(1, 3), (7, 3), (1, 2), (7, 2), (0, 2)]
CROSS = [(1, 0), (7, 0), (1, 1), (7, 1), (0, 0), (0, 1)]
NEAR = SAME + CROSS
FAR_HOPS = [4, 3, 5, 2, 6]
SWEEPS = [2, 0, 1, 3]
ORDER = NEAR + [(hop, side) for side in SWEEPS for hop in FAR_HOPS]
STAGES = [5, 11, 22, 31]
SPLIT = 0


def kernel(
    n_dp, n_mp, act_hbm, wt_hbm, thr_hbm, out_ref,
    act, wt, got, sq_send, sq_got, norm_all, norms, row_send, row_side, row_sum, row_z, tot_send, tot_got,
    limits, scale_a, scale_b, half,
    act_sem, local_sem, bulk_send, bulk_recv, small_send, small_recv, ring_sem, cross_sem, row_sem,
):
    d, m = lax.axis_index("dp"), lax.axis_index("mp")
    cols, outs = wt_hbm.shape
    rows = outs // n_dp
    groups = n_dp // 8
    per_group = cols * 8 // LANES
    chunks = groups * per_group
    steps = act_sem.shape[0]
    tokens = act_hbm.shape[0] // steps
    depth = n_dp // 4
    peers = n_dp - 1

    z, high, core = lax.div(d, 4), lax.rem(lax.div(d, 2), 2), lax.rem(d, 2)
    sides = ((1 - high) * 2 + core, (1 - high) * 2 + 1 - core, high * 2 + 1 - core, high * 2 + core)
    mine = sides[3]
    assert sorted(ORDER) == sorted((hop, side) for hop in range(depth) for side in range(4) if (hop, side) != (0, 3))
    SQUARES, ROW_SIDE, NORM_Z, ROW_Z, NORM_SIDE, TOTAL = range(6)

    def device(hop, side):
        return lax.rem(z + hop, depth) * 4 + sides[side]

    def mp_peer(i):
        return lax.rem(m + i, n_mp)

    def act_copy(i):
        span = pl.ds(pl.multiple_of(i * tokens, tokens), tokens)
        return pltpu.make_async_copy(act_hbm.at[span], act.at[span], act_sem.at[i])

    def block(i):
        return pl.ds(pl.multiple_of(i * rows, rows), rows)

    def place_of(i, n=1):
        return pl.ds(pl.multiple_of(i * cols, 16), n * cols)

    def remote(src, dst, ssem, rsem, to, row=None):
        pltpu.make_async_remote_copy(
            src_ref=src, dst_ref=dst, send_sem=ssem, recv_sem=rsem,
            device_id=(to, m) if row is None else (d, row), device_id_type=MESH,
        ).start()

    def bulk(stage):
        for hop, side in ORDER[STAGES[stage - 1] if stage else 0:STAGES[stage]]:
            to = device(hop, side)
            i = 0 if (hop, side) in NEAR else 1 + side if side < 3 else 4 + FAR_HOPS.index(hop)
            remote((wt_hbm if stage < 2 else wt).at[:, block(to)], got.at[place_of(d)], bulk_send, bulk_recv.at[i], to)

    def to_plane(n, src, dst):
        for side in range(3):
            remote(src(sides[side]), dst, small_send.at[n], small_recv.at[n], device(0, side))

    def to_column(n, src, dst):
        for hop in (4, 3, 5, 2, 6, 1, 7):
            remote(src(lax.rem(z + hop, depth)), dst, small_send.at[n], small_recv.at[n], device(hop, 3))

    def wait_for(ref, sem):
        pltpu.make_async_copy(ref, ref, sem).wait()

    def loop(lo, hi, body):
        lax.fori_loop(lo, hi, lambda i, c: (body(i), c)[1], 0)

    upper, leader = high == 1, m == n_mp - 1

    def signal(sem, to, row=None):
        pl.semaphore_signal(sem, inc=1, device_id=(to, m) if row is None else (d, row), device_id_type=MESH)

    with jax.named_scope("signal"):
        barrier = pltpu.get_barrier_semaphore()
        for hop, side in SAME:
            signal(barrier, device(hop, side))

        @pl.when(jnp.logical_not(upper))
        def _():
            for hop, side in CROSS:
                signal(barrier, device(hop, side))

        @pl.when(jnp.logical_not(leader))
        def _():
            signal(barrier, d, n_mp - 1)

    with jax.named_scope("local"):
        loop(0, steps, lambda i: act_copy(i).start())
        wt_local = pltpu.make_async_copy(wt_hbm, wt, local_sem.at[0])
        wt_local.start()
        own = pltpu.make_async_copy(wt_hbm.at[:, block(d)], got.at[place_of(d)], local_sem.at[1])
        own.start()
        limit_local = pltpu.make_async_copy(thr_hbm, limits, local_sem.at[2])
        limit_local.start()

    def ring_signal(r):
        for hop in (1, depth - 1):
            signal(ring_sem.at[r], device(hop, 3))

    with jax.named_scope("barrier"):
        pl.semaphore_wait(barrier, len(SAME) + len(CROSS) * upper.astype(jnp.int32) + (n_mp - 1) * leader.astype(jnp.int32))
    with jax.named_scope("near"):
        ring_signal(0)
        bulk(0)

        @pl.when(upper)
        def _():
            signal(cross_sem.at[0], device(0, 0))

        @pl.when(leader)
        def _():
            for i in range(1, n_mp):
                signal(row_sem, d, mp_peer(i))

    with jax.named_scope("squares"):
        def add_squares(i, sums):
            act_copy(i).wait()
            base = pl.multiple_of(i * tokens, tokens)
            out = []
            for j in range(chunks):
                x = act[pl.ds(base, tokens), j * LANES:(j + 1) * LANES].astype(jnp.float32)
                out.append(sums[j] + jnp.sum((x * x).reshape(tokens // 8, 8, LANES), axis=0))
            return tuple(out)

        sums = lax.fori_loop(0, SPLIT, add_squares, tuple(jnp.zeros((8, LANES), jnp.float32) for _ in range(chunks)))
        for j in range(chunks):
            half[j] = sums[j]
    with jax.named_scope("ring0"):
        pl.semaphore_wait(ring_sem.at[0], 2)
        ring_signal(1)

        @pl.when(jnp.logical_not(upper))
        def _():
            pl.semaphore_wait(cross_sem.at[0], 1)

        bulk(1)
    with jax.named_scope("squares2"):
        sums = lax.fori_loop(SPLIT, steps, add_squares, tuple(half[j] for j in range(chunks)))
        sums = [jnp.sum(s, axis=0, keepdims=True) for s in sums]
        lane = lax.broadcasted_iota(jnp.int32, (1, LANES), 1)
        for q in range(groups):
            for u in range(8):
                shift = (LANES - cols) * u
                first = sums[per_group * q + max(u - 1, 0)]
                second = sums[per_group * q + min(u, per_group - 1)]
                if u:
                    first = pltpu.roll(first, shift, 1)
                    second = pltpu.roll(second, shift, 1)
                row = jnp.where(lane < shift, first, second)
                sq_send[8 * q + u] = jnp.where(lane < cols, row, 0.0)

    def send_squares(sides_of):
        for side in sides_of:
            for hop in FAR_HOPS + [1, depth - 1, 0]:
                if (hop, side) != (0, 3):
                    to = device(hop, side)
                    remote(sq_send.at[to], sq_got.at[d], small_send.at[SQUARES], small_recv.at[SQUARES], to)

    with jax.named_scope("ring1"):
        pl.semaphore_wait(ring_sem.at[1], 2)
        ring_signal(2)
    with jax.named_scope("ring2"):
        pl.semaphore_wait(ring_sem.at[2], 2)
        signal(cross_sem.at[1], device(0, 0))
        send_squares((2, 3))
    with jax.named_scope("cross"):
        pl.semaphore_wait(cross_sem.at[1], 1)
    with jax.named_scope("issue"):
        send_squares((0, 1))
        wt_local.wait()
        bulk(2)
        sq_got[d] = sq_send[d]

    with jax.named_scope("wait_sq"):
        wait_for(sq_got.at[:peers], small_recv.at[SQUARES])

    with jax.named_scope("rowpart"):
        squares = jnp.sum(sq_got[...].reshape(n_dp // 8, 8, LANES), axis=0)
        squares = jnp.sum(squares, axis=0, keepdims=True)
        norm_lane = jnp.sqrt(squares)
        norm = jnp.broadcast_to(norm_lane, (LANES, LANES)).T[:cols]
        norm_all[mine, z] = norm_lane

        def row_part(r):
            for h in range(rows // LANES):
                w = wt[:, pl.ds(pl.multiple_of(r * rows + h * LANES, LANES), LANES)].astype(jnp.float32)
                part = jnp.sum((jnp.abs(w) * norm).reshape(cols // 8, 8, LANES), axis=0)
                row_send[lax.rem(r, 4), lax.div(r, 4), :, h * LANES:(h + 1) * LANES] = jnp.sum(part, axis=0, keepdims=True)

        loop(0, n_dp, row_part)
    with jax.named_scope("send_row"):
        to_plane(ROW_SIDE, lambda s: row_send.at[s], row_side.at[mine])
        to_column(NORM_Z, lambda p: norm_all.at[mine, z], norm_all.at[mine, z])
        row_side[mine] = row_send[mine]
    with jax.named_scope("wait_row"):
        wait_for(row_side.at[:3], small_recv.at[ROW_SIDE])
    with jax.named_scope("send_row2"):
        row_sum[...] = jnp.sum(row_side[...], axis=0)
        row_z[z] = row_sum[z]
        to_column(ROW_Z, lambda p: row_sum.at[p], row_z.at[z])
        bulk(3)
    with jax.named_scope("wait_norm"):
        wait_for(norm_all.at[0, :depth - 1], small_recv.at[NORM_Z])
        to_plane(NORM_SIDE, lambda s: norm_all.at[mine], norm_all.at[mine])
    with jax.named_scope("wait_row2"):
        wait_for(row_z.at[:depth - 1], small_recv.at[ROW_Z])
    with jax.named_scope("tot"):
        tot_send[...] = jnp.sum(row_z[...], axis=0)

        @pl.when(jnp.logical_not(leader))
        def _():
            pl.semaphore_wait(row_sem, 1)

        for i in range(1, n_mp):
            remote(tot_send, tot_got.at[m], small_send.at[TOTAL], small_recv.at[TOTAL], d, mp_peer(i))
        tot_got[m] = tot_send[...]
    with jax.named_scope("norms"):
        wait_for(norm_all.at[:3], small_recv.at[NORM_SIDE])
        for q in range(groups):
            for t in range(per_group):
                shift = (LANES - cols) * t
                first = norm_all[t % 4, 2 * q + t // 4]
                second = norm_all[(t + 1) % 4, 2 * q + (t + 1) // 4]
                first = pltpu.roll(first, LANES - shift, 1) if shift else first
                second = pltpu.roll(second, cols - shift, 1)
                norms[per_group * q + t] = jnp.where(lane < cols - shift, first, second)
        limit_local.wait()
        own.wait()
    with jax.named_scope("wait_tot"):
        wait_for(tot_got.at[:n_mp - 1], small_recv.at[TOTAL])

    with jax.named_scope("scale"):
        row_mean = jnp.sum(tot_got[...], axis=0) / IN + small_eps
        a = gate_slope / row_mean
        b = 0.5 - gate_slope * limits[...]
        for h in range(rows // LANES):
            part = slice(h * LANES, (h + 1) * LANES)
            scale_a[part] = jnp.broadcast_to(a[:, part], (LANES, LANES)).T
            scale_b[part] = jnp.broadcast_to(b[:, part], (LANES, LANES)).T
        for n, ref in (
            (SQUARES, sq_got.at[:peers]), (ROW_SIDE, row_side.at[:3]), (NORM_Z, norm_all.at[0, :depth - 1]),
            (ROW_Z, row_z.at[:depth - 1]), (NORM_SIDE, norm_all.at[:3]), (TOTAL, tot_got.at[:n_mp - 1]),
        ):
            wait_for(ref, small_send.at[n])

    def finish(j):
        span = pl.ds(pl.multiple_of(j * LANES, LANES), LANES)
        wide = got[span].T.astype(jnp.float32)
        scores = jnp.abs(wide) * norms[j]
        kept = jnp.clip(scores * scale_a[...] + scale_b[...], 0.0, 1.0)
        out_ref[:, span] = (wide * kept).astype(jnp.bfloat16)

    with jax.named_scope("early_wait"):
        wait_for(got.at[place_of(0, len(NEAR))], bulk_recv.at[0])
        for side in range(3):
            wait_for(got.at[place_of(0, len(FAR_HOPS))], bulk_recv.at[1 + side])

    def is_late(s):
        hop = lax.rem(z + depth - lax.div(s, 4), depth)
        return jnp.logical_and(lax.rem(s, 4) == mine, jnp.logical_and(hop > 1, hop < depth - 1))

    def early(j):
        s = lax.div(j, per_group) * 8 + lax.rem(j, per_group)

        @pl.when(jnp.logical_not(jnp.logical_or(is_late(s), is_late(s + 1))))
        def _():
            finish(j)

    with jax.named_scope("early"):
        loop(0, chunks, early)

    for k, hop in enumerate(FAR_HOPS):
        with jax.named_scope("late%d" % k):
            wait_for(got.at[place_of(0)], bulk_recv.at[4 + k])
            s = lax.rem(z + depth - hop, depth) * 4 + mine
            q, u = lax.div(s, 8), lax.rem(s, 8)
            lo, hi = jnp.where(u > 0, u - 1, 0), jnp.where(u < per_group, u + 1, per_group)
            loop(q * per_group + lo, q * per_group + hi, finish)

    with jax.named_scope("drain"):
        wait_for(got.at[place_of(0, peers)], bulk_send)


def solution(mesh):
    n_dp, n_mp = mesh.shape["dp"], mesh.shape["mp"]

    def per_device(activations, weight, thresholds):
        columns = weight.T
        cols, outs = columns.shape
        rows = outs // n_dp
        width = activations.shape[1]
        steps = 8
        depth = n_dp // 4
        dma, regular = pltpu.SemaphoreType.DMA, pltpu.SemaphoreType.REGULAR

        def f32(*shape):
            return pltpu.VMEM(shape, jnp.float32)

        hbm, vmem = pl.BlockSpec(memory_space=pltpu.HBM), pl.BlockSpec(memory_space=pltpu.VMEM)
        return pl.pallas_call(
            functools.partial(kernel, n_dp, n_mp),
            out_shape=pltpu.VMEM((rows, width), jnp.bfloat16),
            in_specs=[hbm, hbm, hbm],
            out_specs=vmem,
            scratch_shapes=[
                pltpu.VMEM(activations.shape, jnp.bfloat16),
                pltpu.VMEM(columns.shape, jnp.bfloat16),
                pltpu.VMEM((n_dp * cols, rows), jnp.bfloat16),
                f32(n_dp, 1, LANES), f32(n_dp, 1, LANES),
                f32(4, depth, 1, LANES), f32(width // LANES, 1, LANES),
                f32(4, depth, 1, rows), f32(4, depth, 1, rows), f32(depth, 1, rows), f32(depth, 1, rows),
                f32(1, rows), f32(n_mp, 1, rows),
                f32(1, rows), f32(rows, LANES), f32(rows, LANES), f32(width // LANES, 8, LANES),
                dma((steps,)), dma((3,)), dma, dma((4 + len(FAR_HOPS),)), dma((6,)), dma((6,)), regular((3,)), regular((2,)), regular,
            ],
            compiler_params=pltpu.CompilerParams(collective_id=0, has_side_effects=True, vmem_limit_bytes=40 * 2**20),
        )(*(pltpu.with_memory_space_constraint(x, pltpu.HBM) for x in (activations, columns, thresholds.reshape(1, rows))))

    placed = (P("dp", "mp"), P(None, ("mp", "dp")), P("dp"))
    return jax.shard_map(per_device, mesh=mesh, in_specs=placed, out_specs=P("dp", "mp"), check_vma=False)
```
